16 devices in a mesh: dp: 2 (over y, z), tp: 8 (over x, core).
Axes of the slice: x: 4, y: 2, z: 1, core: 2. Of those that a mesh axis runs over, the one named last changes fastest.
The devices are a block of a 4x4x8 slice.
Arguments:
- hidden: bfloat16 [512, 1152], P('dp', 'tp'), parts along dimension 0
- cand_ids: int32 [512, 4], P('dp'), parts along dimension 0
- norm_scale: bfloat16 [1152], P('tp')
- emb_table: bfloat16 [262144, 1152], P('tp')
Outputs:
- output 1: float32 [512], P('dp'), parts along dimension 0
- output 2: float32 [512, 4], P('dp'), parts along dimension 0
- output 3: bfloat16 [512, 262144], P('dp', 'tp'), parts along dimension 0
There are 2 independent parts. The reference program is written for one: setup_inputs(seed, part) draws one part's arguments, and reference() takes and returns one part's arrays. A program takes and returns all parts, laid end to end along the dimension named above; an argument that names none is the same for every part.
All inputs are finite; a program needn't handle non-finite values.
Results may differ from the reference program's by a relative error of at most 0.001.
Values are sent between devices in bfloat16 or wider.
A program may use at most 768 MiB of HBM per device.

```python
import jax
import jax.numpy as jnp
from jax import lax

BATCH = 256
D = 1152
V = 262144
CANDIDATES = 4
TABLE_BLOCKS = 64
NORM_EPS = 1e-6
SOFT_CAP = 30.0


def draw_table(key):
    block_keys = jax.random.split(key, TABLE_BLOCKS)

    def one_block(blk_key):
        block_vals = jax.random.normal(blk_key, (V // TABLE_BLOCKS, D), jnp.float32)
        return (block_vals * (10.0 * D ** -0.5)).astype(jnp.bfloat16)

    return lax.map(one_block, block_keys).reshape(V, D)


def setup_inputs(seed: int = 0, part: int = 0) -> dict:
    part_key = jax.random.fold_in(jax.random.key(seed), part)
    key_hidden, key_rows, key_cand = jax.random.split(part_key, 3)
    key_scale, key_table = jax.random.split(jax.random.key(seed + 1))
    col_gain = jnp.exp(jnp.linspace(-1.0, 1.0, D))
    row_gain = jnp.exp(jax.random.uniform(key_rows, (BATCH, 1), jnp.float32, -0.5, 0.5))
    hidden = (jax.random.normal(key_hidden, (BATCH, D), jnp.float32) * col_gain * row_gain).astype(jnp.bfloat16)
    cand_ids = jax.random.randint(key_cand, (BATCH, CANDIDATES), 0, V, jnp.int32)
    cand_ids = cand_ids.at[0, 0].set(0).at[BATCH - 1, CANDIDATES - 1].set(V - 1)
    norm_scale = (0.5 * jax.random.normal(key_scale, (D,), jnp.float32)).astype(jnp.bfloat16)
    emb_table = draw_table(key_table)
    return {"hidden": hidden, "cand_ids": cand_ids, "norm_scale": norm_scale, "emb_table": emb_table}


def reference(hidden, cand_ids, norm_scale, emb_table):
    hidden_f32 = hidden.astype(jnp.float32)
    mean_sq = jnp.mean(hidden_f32 * hidden_f32, axis=1, keepdims=True)
    normed = (hidden_f32 * lax.rsqrt(mean_sq + NORM_EPS) * (1.0 + norm_scale.astype(jnp.float32))).astype(jnp.bfloat16)
    logits = jnp.dot(normed, emb_table.T, preferred_element_type=jnp.float32)
    capped = SOFT_CAP * jnp.tanh(logits / SOFT_CAP)
    row_max = jnp.max(capped, axis=1, keepdims=True)
    row_lse = row_max[:, 0] + jnp.log(jnp.sum(jnp.exp(capped - row_max), axis=1))
    log_probs = capped - row_lse[:, None]
    cand_logp = jnp.take_along_axis(log_probs, cand_ids, axis=1)
    return row_lse, cand_logp, log_probs.astype(jnp.bfloat16)
```

```python
import functools
import math

import jax
import jax.numpy as jnp
from jax import lax
from jax.experimental import pallas as pl
from jax.experimental.pallas import tpu as pltpu
from jax.sharding import PartitionSpec as P

NORM_EPS = 1e-6
SOFT_CAP = 30.0
LOG2E = math.log2(math.e)
CHUNK = 1024
RING = 10
OUT_ROWS = 16
OUT_RING = 4
MESH = pl.DeviceIdType.MESH


def head_kernel(n, h_hbm, s_hbm, ids_ref, tab_hbm, c_ref, tail_ref,
                ebuf, gath, s_all, s_col, normed, z_a, z_b, stats,
                e_sem, in_sem, s_sem, s_recv, own_send, own_recv, far_send, far_recv,
                relay_send, relay_recv, st_send, st_recv):
    me = lax.axis_index("tp")
    core = lax.rem(me, 2)
    mate = me + 1 - 2 * core
    chips = n // 2
    vocab, width = tab_hbm.shape
    rows = normed.shape[1]
    feat = h_hbm.shape[0]
    n_chunks = vocab // CHUNK

    def far(d):
        return lax.rem(me + 2 * d, n)

    def from_far(d):
        return lax.rem(me + n - 2 * d, n)

    def table_copy(j):
        slot = lax.rem(j, RING)
        return pltpu.make_async_copy(
            tab_hbm.at[pl.ds(pl.multiple_of(j * CHUNK, CHUNK), CHUNK), :],
            ebuf.at[slot], e_sem.at[slot])

    def remote(src, dst, send, recv, peer):
        return pltpu.make_async_remote_copy(
            src_ref=src, dst_ref=dst, send_sem=send, recv_sem=recv,
            device_id={"tp": peer}, device_id_type=MESH)

    h_in = pltpu.make_async_copy(h_hbm, gath.at[me], in_sem.at[0])
    s_in = pltpu.make_async_copy(s_hbm, s_all.at[me], in_sem.at[1])
    h_in.start()
    s_in.start()
    barrier = pltpu.get_barrier_semaphore()
    for d in range(1, n):
        pl.semaphore_signal(barrier, inc=1, device_id={"tp": lax.rem(me + d, n)}, device_id_type=MESH)
    for j in range(RING):
        table_copy(j).start()
    s_in.wait()
    h_in.wait()
    pl.semaphore_wait(barrier, n - 1)

    far_copies = [remote(gath.at[me], gath.at[me], far_send.at[d - 1], far_recv.at[d - 1], far(d)) for d in range(1, chips)]
    own_copy = remote(gath.at[me], gath.at[me], own_send, own_recv, mate)
    s_copies = [remote(s_all.at[me], s_all.at[me], s_sem.at[d - 1], s_recv.at[d - 1], lax.rem(me + d, n)) for d in range(1, n)]
    for cp in s_copies:
        cp.start()
    for cp in far_copies:
        cp.start()
    own_copy.start()

    for cp in s_copies:
        cp.wait()
    for d in range(n):
        s_row = 1.0 + s_all[d].astype(jnp.float32)
        pad = jnp.zeros((1, 256 - feat), jnp.float32)
        s_wide = jnp.broadcast_to(jnp.concatenate([s_row, pad], axis=1), (128, 256))
        s_col[d * feat:(d + 1) * feat, :] = s_wide.T[:feat, :]

    relays = []
    order = sorted(range(1, chips), key=lambda d: min(d, chips - d))
    for d in order:
        far_copies[d - 1].wait_recv()
        src = from_far(d)
        cp = remote(gath.at[src], gath.at[src], relay_send.at[d - 1], relay_recv.at[d - 1], mate)
        cp.start()
        relays.append(cp)
    own_copy.wait()
    for cp in relays:
        cp.wait_recv()

    sq = jnp.zeros((8, rows), jnp.float32)
    for d in range(n):
        h32 = gath[d].astype(jnp.float32)
        sq = sq + jnp.sum((h32 * h32).reshape(feat // 8, 8, rows), axis=0)
    mean_sq = jnp.sum(sq, axis=0, keepdims=True) / width
    inv = lax.rsqrt(mean_sq + NORM_EPS)
    for d in range(n):
        scale = s_col[d * feat:(d + 1) * feat, :]
        scale = jnp.concatenate([scale] * (rows // 128), axis=1)
        normed[d * feat:(d + 1) * feat, :] = (gath[d].astype(jnp.float32) * inv * scale).astype(jnp.bfloat16)
    for cp in far_copies:
        cp.wait_send()
    for cp in relays:
        cp.wait_send()

    def multiply(j, z_ref):
        z_ref[...] = jnp.dot(ebuf[lax.rem(j, RING)], normed[...], preferred_element_type=jnp.float32)

    n_cand = ids_ref.shape[0]
    first = me * vocab
    sub = lax.broadcasted_iota(jnp.int32, (8, rows), 0)

    def finish(j, z_ref, carry):
        acc, picks = carry[0], list(carry[1:])
        want = [ids_ref[k:k + 1, :] - (first + j * CHUNK) - sub for k in range(n_cand)]
        for b in range(CHUNK // 128):
            x = z_ref[b * 128:(b + 1) * 128, :]
            t = jnp.tanh(x * (1.0 / SOFT_CAP))
            e = jnp.exp2(t * (SOFT_CAP * LOG2E))
            acc = acc + jnp.sum(e.reshape(16, 8, rows), axis=0)
            c = t * SOFT_CAP
            for g in range(16):
                part = c[g * 8:(g + 1) * 8, :]
                for k in range(n_cand):
                    picks[k] = jnp.where(want[k] == b * 128 + g * 8, part, picks[k])
            c_ref[:, pl.ds(pl.multiple_of(j * CHUNK + b * 128, 128), 128)] = c.T
        return (acc, *picks)

    table_copy(0).wait()
    multiply(0, z_a)

    def pair(p, acc):
        a = 2 * p
        for k in (1, 2):
            table_copy(a + k).wait()
        for k in (-1, 0):
            nxt = a + k + RING

            @pl.when((nxt >= RING) & (nxt < n_chunks))
            def _():
                table_copy(nxt).start()
        multiply(a + 1, z_b)
        acc = finish(a, z_a, acc)
        multiply(a + 2, z_a)
        return finish(a + 1, z_b, acc)

    acc = lax.fori_loop(0, n_chunks // 2 - 1, pair, (jnp.zeros((8, rows), jnp.float32),) * (1 + n_cand))
    table_copy(n_chunks - 1).wait()
    multiply(n_chunks - 1, z_b)
    acc = finish(n_chunks - 2, z_a, acc)
    acc = finish(n_chunks - 1, z_b, acc)

    for k, part in enumerate(acc):
        stats[me, k:k + 1, :] = jnp.sum(part, axis=0, keepdims=True)
    st_copies = [remote(stats.at[me], stats.at[me], st_send.at[d - 1], st_recv.at[d - 1], lax.rem(me + d, n)) for d in range(1, n)]
    for cp in st_copies:
        cp.start()
    for cp in st_copies:
        cp.wait()
    total = stats[0]
    for d in range(1, n):
        total = total + stats[d]
    lse = jnp.log(total[0:1, :])
    tail_ref[0:1, :] = lse
    tail_ref[1:1 + n_cand, :] = total[1:1 + n_cand, :] - lse


def write_kernel(c_ref, tail_ref, lse_ref, cand_ref, out_hbm, l_col, obuf, o_sem):
    rows, vocab = c_ref.shape
    lse_ref[...] = tail_ref[0:1, :]
    cand_ref[...] = tail_ref[1:1 + cand_ref.shape[0], :]
    for b in range(rows // 128):
        l_col[b * 128:(b + 1) * 128, :] = jnp.broadcast_to(tail_ref[0:1, b * 128:(b + 1) * 128], (128, 128)).T
    n_blk = rows // OUT_ROWS

    def out_copy(i, slot):
        return pltpu.make_async_copy(
            obuf.at[slot], out_hbm.at[pl.ds(pl.multiple_of(i * OUT_ROWS, OUT_ROWS), OUT_ROWS), :], o_sem.at[slot])

    def block(i, carry):
        slot = lax.rem(i, OUT_RING)

        @pl.when(i >= OUT_RING)
        def _():
            out_copy(i - OUT_RING, slot).wait()
        r0 = pl.multiple_of(i * OUT_ROWS, OUT_ROWS)
        col = l_col[pl.ds(r0, OUT_ROWS), :]
        step = 2048

        def part(q, c):
            v0 = pl.multiple_of(q * step, step)
            lse = jnp.concatenate([col] * (step // 128), axis=1)
            obuf[slot, :, pl.ds(v0, step)] = (c_ref[pl.ds(r0, OUT_ROWS), pl.ds(v0, step)] - lse).astype(jnp.bfloat16)
            return c

        lax.fori_loop(0, vocab // step, part, 0)
        out_copy(i, slot).start()
        return carry

    lax.fori_loop(0, n_blk, block, 0)
    for i in range(n_blk - OUT_RING, n_blk):
        out_copy(i, i % OUT_RING).wait()


def solution(mesh):
    n = mesh.shape["tp"]

    def device_step(hidden_blk, cand_ids, scale_blk, table_blk):
        rows, feat = hidden_blk.shape
        vocab, width = table_blk.shape
        n_cand = cand_ids.shape[1]
        ids_t = cand_ids.T
        dma = pltpu.SemaphoreType.DMA
        any_space = pl.BlockSpec(memory_space=pl.ANY)
        vmem = pl.BlockSpec(memory_space=pltpu.VMEM)
        capped, tail = pl.pallas_call(
            functools.partial(head_kernel, n),
            out_shape=(pltpu.VMEM((rows, vocab), jnp.float32),
                       jax.ShapeDtypeStruct((8, rows), jnp.float32)),
            in_specs=[any_space, any_space, vmem, any_space],
            out_specs=(vmem, vmem),
            scratch_shapes=[
                pltpu.VMEM((RING, CHUNK, width), jnp.bfloat16),
                pltpu.VMEM((n, feat, rows), jnp.bfloat16),
                pltpu.VMEM((n, 1, feat), jnp.bfloat16),
                pltpu.VMEM((n * feat, 128), jnp.float32),
                pltpu.VMEM((n * feat, rows), jnp.bfloat16),
                pltpu.VMEM((CHUNK, rows), jnp.float32),
                pltpu.VMEM((CHUNK, rows), jnp.float32),
                pltpu.VMEM((n, 8, rows), jnp.float32),
                dma((RING,)), dma((2,)), dma((n - 1,)), dma((n - 1,)), dma, dma,
                dma((n // 2 - 1,)), dma((n // 2 - 1,)), dma((n // 2 - 1,)), dma((n // 2 - 1,)),
                dma((n - 1,)), dma((n - 1,)),
            ],
            compiler_params=pltpu.CompilerParams(
                collective_id=0, has_side_effects=True, vmem_limit_bytes=31 * 2**20),
        )(hidden_blk.T, scale_blk.reshape(1, feat), ids_t, table_blk)
        lse, cand, logp = pl.pallas_call(
            write_kernel,
            out_shape=(jax.ShapeDtypeStruct((1, rows), jnp.float32),
                       jax.ShapeDtypeStruct((n_cand, rows), jnp.float32),
                       jax.ShapeDtypeStruct((rows, vocab), jnp.bfloat16)),
            in_specs=[vmem, vmem],
            out_specs=(vmem, vmem, any_space),
            scratch_shapes=[pltpu.VMEM((rows, 128), jnp.float32),
                            pltpu.VMEM((OUT_RING, OUT_ROWS, vocab), jnp.bfloat16),
                            dma((OUT_RING,))],
            compiler_params=pltpu.CompilerParams(vmem_limit_bytes=31 * 2**20),
        )(pltpu.with_memory_space_constraint(capped, pltpu.VMEM), tail)
        return lse.reshape(rows), cand.T, logp

    return jax.shard_map(
        device_step,
        mesh=mesh,
        in_specs=(P("dp", "tp"), P("dp", None), P("tp"), P("tp", None)),
        out_specs=(P("dp"), P("dp", None), P("dp", "tp")),
        check_vma=False,
    )
```

```python
import functools
import math

import jax
import jax.numpy as jnp
from jax import lax
from jax.experimental import pallas as pl
from jax.experimental.pallas import tpu as pltpu
from jax.sharding import PartitionSpec as P

NORM_EPS = 1e-6
SOFT_CAP = 30.0
LOG2E = math.log2(math.e)
CHUNK = 1024
RING = 10
OUT_ROWS = 16
OUT_RING = 4
MESH = pl.DeviceIdType.MESH


def head_kernel(n, h_hbm, s_hbm, ids_hbm, tab_hbm, c_ref, tail_ref,
                ebuf, gath, s_own, s_all, s_col, sq_part, normed, z_a, z_b, ids_ref, stats,
                e_sem, in_sem, s_send, s_recv, h_send, h_recv, mate_send, mate_recv, st_send, st_recv):
    me = lax.axis_index("tp")
    core = lax.rem(me, 2)
    mate = me + 1 - 2 * core
    vocab, width = tab_hbm.shape
    feat, rows = h_hbm.shape
    halves = gath.shape[1]
    n_chunks = vocab // CHUNK
    n_cand = ids_hbm.shape[0]

    onward = lax.rem(me + 2 + core * (n - 4), n)
    behind = lax.rem(me + n - 2 - core * (n - 4), n)
    across = lax.rem(me + 4, n)

    def table_copy(j):
        slot = lax.rem(j, RING)
        return pltpu.make_async_copy(
            tab_hbm.at[pl.ds(pl.multiple_of(j * CHUNK, CHUNK), CHUNK), :],
            ebuf.at[slot], e_sem.at[slot])

    def remote(ref, send, recv, peer):
        return pltpu.make_async_remote_copy(
            src_ref=ref, dst_ref=ref, send_sem=send, recv_sem=recv,
            device_id={"tp": peer}, device_id_type=MESH)

    h_in = [pltpu.make_async_copy(h_hbm.at[:, pl.ds(q * 128, 128)], gath.at[me, q], in_sem.at[q]) for q in range(halves)]
    s_in = pltpu.make_async_copy(s_hbm, s_own, in_sem.at[halves])
    i_in = pltpu.make_async_copy(ids_hbm, ids_ref, in_sem.at[halves + 1])
    for cp in h_in + [s_in, i_in]:
        cp.start()
    barrier = pltpu.get_barrier_semaphore()
    for d in range(1, n):
        pl.semaphore_signal(barrier, inc=1, device_id={"tp": lax.rem(me + d, n)}, device_id_type=MESH)
    for j in range(RING):
        table_copy(j).start()
    s_in.wait()
    s_all[me] = s_own[...].astype(jnp.float32).reshape(1, feat)
    i_in.wait()
    for cp in h_in:
        cp.wait()
    pl.semaphore_wait(barrier, n - 1)

    def hop(src, leg, q, peer):
        return remote(gath.at[src, q], h_send.at[leg, q], h_recv.at[leg, q], peer)

    def to_mate(src, leg, q):
        return remote(gath.at[src, q], mate_send.at[leg, q], mate_recv.at[leg, q], mate)

    s_copies = [remote(s_all.at[me], s_send.at[d - 1], s_recv.at[d - 1], lax.rem(me + d, n)) for d in range(1, n)]
    sent = []

    def send(cp):
        cp.start()
        sent.append(cp)

    for q in range(halves):
        send(hop(me, 0, q, onward))
        send(hop(me, 1, q, behind))
    for cp in s_copies:
        send(cp)
    for q in range(halves):
        send(to_mate(me, 0, q))

    def squares(d):
        h32 = gath[d].astype(jnp.float32)
        h2 = jnp.sum((h32 * h32).reshape(halves, feat // 8, 8, 128), axis=1)
        for q in range(halves):
            sq_part[d, :, q * 128:(q + 1) * 128] = h2[q]

    for q in range(halves):
        hop(behind, 0, q, onward).wait_recv()
        send(hop(behind, 2, q, onward))
        send(to_mate(behind, 1, q))
        hop(onward, 1, q, behind).wait_recv()
        send(to_mate(onward, 2, q))
    squares(me)
    squares(behind)
    squares(onward)
    for cp in s_copies:
        cp.wait_recv()
    for d in range(n):
        pad = jnp.zeros((1, 256 - feat), jnp.float32)
        s_wide = jnp.broadcast_to(jnp.concatenate([1.0 + s_all[d], pad], axis=1), (128, 256))
        s_col[d * feat:(d + 1) * feat, :] = s_wide.T[:feat, :]
    for leg, src in ((0, mate), (1, onward + 1 - 2 * core), (2, behind + 1 - 2 * core)):
        for q in range(halves):
            to_mate(src, leg, q).wait_recv()
    for d in (0, 2, n - 2):
        squares(lax.rem(mate + d, n))
    for q in range(halves):
        hop(across, 2, q, onward).wait_recv()
        send(to_mate(across, 3, q))
    squares(across)
    far = lax.rem(mate + 4, n)
    for q in range(halves):
        to_mate(far, 3, q).wait_recv()
    squares(far)

    sq = sq_part[0]
    for d in range(1, n):
        sq = sq + sq_part[d]
    inv = lax.rsqrt(jnp.sum(sq, axis=0, keepdims=True) / width + NORM_EPS)
    for d in range(n):
        scale = s_col[d * feat:(d + 1) * feat, :]
        for q in range(halves):
            cols = slice(q * 128, (q + 1) * 128)
            normed[d * feat:(d + 1) * feat, cols] = (gath[d, q].astype(jnp.float32) * inv[:, cols] * scale).astype(jnp.bfloat16)
    for cp in sent:
        cp.wait_send()

    def multiply(j, z_ref):
        z_ref[...] = jnp.dot(ebuf[lax.rem(j, RING)], normed[...], preferred_element_type=jnp.float32)

    first = me * vocab
    sub = lax.broadcasted_iota(jnp.int32, (8, rows), 0)

    def finish(j, z_ref, carry):
        acc, picks = carry[0], list(carry[1:])
        want = [ids_ref[k:k + 1, :] - (first + j * CHUNK) - sub for k in range(n_cand)]
        for b in range(CHUNK // 128):
            x = z_ref[b * 128:(b + 1) * 128, :]
            t = jnp.tanh(x * (1.0 / SOFT_CAP))
            e = jnp.exp2(t * (SOFT_CAP * LOG2E))
            acc = acc + jnp.sum(e.reshape(16, 8, rows), axis=0)
            c = t * SOFT_CAP
            for g in range(16):
                part = c[g * 8:(g + 1) * 8, :]
                for k in range(n_cand):
                    picks[k] = jnp.where(want[k] == b * 128 + g * 8, part, picks[k])
            c_ref[:, pl.ds(pl.multiple_of(j * CHUNK + b * 128, 128), 128)] = c.T
        return (acc, *picks)

    table_copy(0).wait()
    multiply(0, z_a)

    def pair(p, acc):
        a = 2 * p
        for k in (1, 2):
            table_copy(a + k).wait()
        for k in (-1, 0):
            nxt = a + k + RING

            @pl.when((nxt >= RING) & (nxt < n_chunks))
            def _():
                table_copy(nxt).start()
        multiply(a + 1, z_b)
        acc = finish(a, z_a, acc)
        multiply(a + 2, z_a)
        return finish(a + 1, z_b, acc)

    acc = lax.fori_loop(0, n_chunks // 2 - 1, pair, (jnp.zeros((8, rows), jnp.float32),) * (1 + n_cand))
    table_copy(n_chunks - 1).wait()
    multiply(n_chunks - 1, z_b)
    acc = finish(n_chunks - 2, z_a, acc)
    acc = finish(n_chunks - 1, z_b, acc)

    for k, part in enumerate(acc):
        stats[me, k:k + 1, :] = jnp.sum(part, axis=0, keepdims=True)
    st_copies = [remote(stats.at[me], st_send.at[d - 1], st_recv.at[d - 1], lax.rem(me + d, n)) for d in range(1, n)]
    for cp in st_copies:
        cp.start()
    for cp in st_copies:
        cp.wait()
    total = stats[0]
    for d in range(1, n):
        total = total + stats[d]
    lse = jnp.log(total[0:1, :])
    tail_ref[0:1, :] = lse
    tail_ref[1:1 + n_cand, :] = total[1:1 + n_cand, :] - lse


def write_kernel(c_ref, tail_ref, lse_hbm, cand_hbm, out_hbm, lse_buf, cand_buf, l_col, obuf, o_sem, t_sem):
    rows, vocab = c_ref.shape
    lse_buf[...] = tail_ref[0:1, :]
    cand_buf[...] = tail_ref[1:1 + cand_buf.shape[0], :]
    for b in range(rows // 128):
        l_col[b * 128:(b + 1) * 128, :] = jnp.broadcast_to(tail_ref[0:1, b * 128:(b + 1) * 128], (128, 128)).T
    small = [pltpu.make_async_copy(lse_buf, lse_hbm, t_sem.at[0]), pltpu.make_async_copy(cand_buf, cand_hbm, t_sem.at[1])]
    for cp in small:
        cp.start()
    n_blk = rows // OUT_ROWS

    def out_copy(i, slot):
        return pltpu.make_async_copy(
            obuf.at[slot], out_hbm.at[pl.ds(pl.multiple_of(i * OUT_ROWS, OUT_ROWS), OUT_ROWS), :], o_sem.at[slot])

    def block(i, carry):
        slot = lax.rem(i, OUT_RING)

        @pl.when(i >= OUT_RING)
        def _():
            out_copy(i - OUT_RING, slot).wait()
        r0 = pl.multiple_of(i * OUT_ROWS, OUT_ROWS)
        col = l_col[pl.ds(r0, OUT_ROWS), :]
        step = 2048

        def part(q, c):
            v0 = pl.multiple_of(q * step, step)
            lse = jnp.concatenate([col] * (step // 128), axis=1)
            obuf[slot, :, pl.ds(v0, step)] = (c_ref[pl.ds(r0, OUT_ROWS), pl.ds(v0, step)] - lse).astype(jnp.bfloat16)
            return c

        lax.fori_loop(0, vocab // step, part, 0)
        out_copy(i, slot).start()
        return carry

    lax.fori_loop(0, n_blk, block, 0)
    for i in range(n_blk - OUT_RING, n_blk):
        out_copy(i, i % OUT_RING).wait()
    for cp in small:
        cp.wait()


def solution(mesh):
    n = mesh.shape["tp"]

    def device_step(hidden_blk, cand_ids, scale_blk, table_blk):
        rows, feat = hidden_blk.shape
        vocab, width = table_blk.shape
        n_cand = cand_ids.shape[1]
        ids_t = cand_ids.T
        dma = pltpu.SemaphoreType.DMA
        any_space = pl.BlockSpec(memory_space=pl.ANY)
        vmem = pl.BlockSpec(memory_space=pltpu.VMEM)
        capped, tail = pl.pallas_call(
            functools.partial(head_kernel, n),
            out_shape=(pltpu.VMEM((rows, vocab), jnp.float32),
                       pltpu.VMEM((8, rows), jnp.float32)),
            in_specs=[any_space] * 4,
            out_specs=(vmem, vmem),
            scratch_shapes=[
                pltpu.VMEM((RING, CHUNK, width), jnp.bfloat16),
                pltpu.VMEM((n, rows // 128, feat, 128), jnp.bfloat16),
                pltpu.VMEM((feat,), jnp.bfloat16),
                pltpu.VMEM((n, 1, feat), jnp.float32),
                pltpu.VMEM((n * feat, 128), jnp.float32),
                pltpu.VMEM((n, 8, rows), jnp.float32),
                pltpu.VMEM((n * feat, rows), jnp.bfloat16),
                pltpu.VMEM((CHUNK, rows), jnp.float32),
                pltpu.VMEM((CHUNK, rows), jnp.float32),
                pltpu.VMEM((n_cand, rows), jnp.int32),
                pltpu.VMEM((n, 8, rows), jnp.float32),
                dma((RING,)), dma((rows // 128 + 2,)), dma((n - 1,)), dma((n - 1,)),
                dma((3, rows // 128)), dma((3, rows // 128)), dma((4, rows // 128)), dma((4, rows // 128)),
                dma((n - 1,)), dma((n - 1,)),
            ],
            compiler_params=pltpu.CompilerParams(
                collective_id=0, has_side_effects=True, vmem_limit_bytes=31 * 2**20),
        )(hidden_blk.T, scale_blk, ids_t, table_blk)
        lse, cand, logp = pl.pallas_call(
            write_kernel,
            out_shape=(jax.ShapeDtypeStruct((1, rows), jnp.float32),
                       jax.ShapeDtypeStruct((n_cand, rows), jnp.float32),
                       jax.ShapeDtypeStruct((rows, vocab), jnp.bfloat16)),
            in_specs=[vmem, vmem],
            out_specs=(any_space,) * 3,
            scratch_shapes=[pltpu.VMEM((1, rows), jnp.float32),
                            pltpu.VMEM((n_cand, rows), jnp.float32),
                            pltpu.VMEM((rows, 128), jnp.float32),
                            pltpu.VMEM((OUT_RING, OUT_ROWS, vocab), jnp.bfloat16),
                            dma((OUT_RING,)), dma((2,))],
            compiler_params=pltpu.CompilerParams(vmem_limit_bytes=31 * 2**20),
        )(pltpu.with_memory_space_constraint(capped, pltpu.VMEM),
          pltpu.with_memory_space_constraint(tail, pltpu.VMEM))
        return lse.reshape(rows), cand.T, logp

    return jax.shard_map(
        device_step,
        mesh=mesh,
        in_specs=(P("dp", "tp"), P("dp", None), P("tp"), P("tp", None)),
        out_specs=(P("dp"), P("dp", None), P("dp", "tp")),
        check_vma=False,
    )
```

```python
import functools
import math

import jax
import jax.numpy as jnp
from jax import lax
from jax.experimental import pallas as pl
from jax.experimental.pallas import tpu as pltpu
from jax.sharding import PartitionSpec as P

NORM_EPS = 1e-6
SOFT_CAP = 30.0
LOG2E = math.log2(math.e)
CHUNK = 1024
RING = 10
OUT_ROWS = 16
OUT_RING = 4
MESH = pl.DeviceIdType.MESH


def head_kernel(n, h_hbm, s_hbm, ids_hbm, tab_hbm, t_ref, tail_ref,
                ebuf, gath, s_own, s_all, s_col, sq_part, normed, z_a, z_b, ids_sm, ids_ref, ids_blk, picked, stats,
                e_sem, in_sem, s_send, s_recv, h_send, h_recv, mate_send, mate_recv, st_send, st_recv):
    me = lax.axis_index("tp")
    core = lax.rem(me, 2)
    mate = me + 1 - 2 * core
    vocab, width = tab_hbm.shape
    feat, rows = h_hbm.shape
    halves = gath.shape[1]
    n_chunks = vocab // CHUNK
    n_cand = ids_hbm.shape[0]

    onward = lax.rem(me + 2 + core * (n - 4), n)
    behind = lax.rem(me + n - 2 - core * (n - 4), n)
    across = lax.rem(me + 4, n)

    def table_copy(j):
        slot = lax.rem(j, RING)
        return pltpu.make_async_copy(
            tab_hbm.at[pl.ds(pl.multiple_of(j * CHUNK, CHUNK), CHUNK), :],
            ebuf.at[slot], e_sem.at[slot])

    def remote(ref, send, recv, peer):
        return pltpu.make_async_remote_copy(
            src_ref=ref, dst_ref=ref, send_sem=send, recv_sem=recv,
            device_id={"tp": peer}, device_id_type=MESH)

    h_in = [pltpu.make_async_copy(h_hbm.at[:, pl.ds(q * 128, 128)], gath.at[me, q], in_sem.at[q]) for q in range(halves)]
    s_in = pltpu.make_async_copy(s_hbm, s_own, in_sem.at[halves])
    i_in = pltpu.make_async_copy(ids_hbm, ids_ref, in_sem.at[halves + 1])
    for cp in h_in + [s_in, i_in]:
        cp.start()
    barrier = pltpu.get_barrier_semaphore()
    first = me * vocab
    for d in range(1, n):
        pl.semaphore_signal(barrier, inc=1, device_id={"tp": lax.rem(me + d, n)}, device_id_type=MESH)
    for j in range(RING):
        table_copy(j).start()
    s_in.wait()
    s_all[me] = s_own[...].astype(jnp.float32).reshape(1, feat)
    i_in.wait()
    for cp in h_in:
        cp.wait()
    pl.semaphore_wait(barrier, n - 1)

    def hop(src, leg, q, peer):
        return remote(gath.at[src, q], h_send.at[leg, q], h_recv.at[leg, q], peer)

    def to_mate(src, leg, q):
        return remote(gath.at[src, q], mate_send.at[leg, q], mate_recv.at[leg, q], mate)

    s_copies = [remote(s_all.at[me], s_send.at[d - 1], s_recv.at[d - 1], lax.rem(me + d, n)) for d in range(1, n)]
    sent = []

    def send(cp):
        cp.start()
        sent.append(cp)

    for q in range(halves):
        send(hop(me, 0, q, onward))
        send(hop(me, 1, q, behind))
    for cp in s_copies:
        send(cp)
    for q in range(halves):
        send(to_mate(me, 0, q))

    def squares(d):
        h32 = gath[d].astype(jnp.float32)
        h2 = jnp.sum((h32 * h32).reshape(halves, feat // 8, 8, 128), axis=1)
        for q in range(halves):
            sq_part[d, :, q * 128:(q + 1) * 128] = h2[q]

    for q in range(halves):
        hop(behind, 0, q, onward).wait_recv()
        send(hop(behind, 2, q, onward))
        send(to_mate(behind, 1, q))
        hop(onward, 1, q, behind).wait_recv()
        send(to_mate(onward, 2, q))
    block_of = lax.max(lax.min(lax.shift_right_arithmetic(ids_ref[...] - first, 7), vocab // 128 - 1), 0)
    ids_blk[...] = block_of
    squares(me)
    squares(behind)
    squares(onward)
    for cp in s_copies:
        cp.wait_recv()
    for d in range(n):
        pad = jnp.zeros((1, 256 - feat), jnp.float32)
        s_wide = jnp.broadcast_to(jnp.concatenate([1.0 + s_all[d], pad], axis=1), (128, 256))
        s_col[d * feat:(d + 1) * feat, :] = s_wide.T[:feat, :]
    for leg, src in ((0, mate), (1, onward + 1 - 2 * core), (2, behind + 1 - 2 * core)):
        for q in range(halves):
            to_mate(src, leg, q).wait_recv()
    for d in (0, 2, n - 2):
        squares(lax.rem(mate + d, n))
    for q in range(halves):
        hop(across, 2, q, onward).wait_recv()
        send(to_mate(across, 3, q))
    squares(across)
    far = lax.rem(mate + 4, n)
    for q in range(halves):
        to_mate(far, 3, q).wait_recv()
    squares(far)

    sq = sq_part[0]
    for d in range(1, n):
        sq = sq + sq_part[d]
    inv = lax.rsqrt(jnp.sum(sq, axis=0, keepdims=True) / width + NORM_EPS)
    for d in range(n):
        scale = s_col[d * feat:(d + 1) * feat, :]
        for q in range(halves):
            cols = slice(q * 128, (q + 1) * 128)
            normed[d * feat:(d + 1) * feat, cols] = (gath[d, q].astype(jnp.float32) * inv[:, cols] * scale).astype(jnp.bfloat16)
    to_smem = pltpu.make_async_copy(ids_blk, ids_sm, in_sem.at[halves + 2])
    to_smem.start()

    def multiply(j, z_ref):
        z_ref[...] = jnp.dot(ebuf[lax.rem(j, RING)], normed[...], preferred_element_type=jnp.float32)

    def finish(j, z_ref, acc):
        for b in range(CHUNK // 128):
            t = jnp.tanh(z_ref[b * 128:(b + 1) * 128, :] * (1.0 / SOFT_CAP))
            e = jnp.exp2(t * (SOFT_CAP * LOG2E))
            acc = acc + jnp.sum(e.reshape(16, 8, rows), axis=0)
            t_ref[j * (CHUNK // 128) + b] = t.T.reshape(rows // 8, 8, 128)
        return acc

    table_copy(0).wait()
    multiply(0, z_a)

    def pair(p, acc):
        a = 2 * p
        for k in (1, 2):
            table_copy(a + k).wait()
        for k in (-1, 0):
            nxt = a + k + RING

            @pl.when((nxt >= RING) & (nxt < n_chunks))
            def _():
                table_copy(nxt).start()
        multiply(a + 1, z_b)
        acc = finish(a, z_a, acc)
        multiply(a + 2, z_a)
        return finish(a + 1, z_b, acc)

    acc = lax.fori_loop(0, n_chunks // 2 - 1, pair, jnp.zeros((8, rows), jnp.float32))
    table_copy(n_chunks - 1).wait()
    multiply(n_chunks - 1, z_b)
    acc = finish(n_chunks - 2, z_a, acc)
    acc = finish(n_chunks - 1, z_b, acc)

    stats[me, 0:1, :] = jnp.sum(acc, axis=0, keepdims=True)
    sub = lax.broadcasted_iota(jnp.int32, (8, 128), 0)

    to_smem.wait()

    def pick(g, carry):
        for k in range(n_cand):
            tile = jnp.zeros((8, 128), jnp.float32)
            for r in range(8):
                tile = jnp.where(sub == r, t_ref[ids_sm[k, g * 8 + r], g], tile)
            picked[k, g] = tile
        return carry

    lax.fori_loop(0, rows // 8, pick, 0)
    lane = lax.broadcasted_iota(jnp.int32, (128, rows), 0)
    for k in range(n_cand):
        loc = ids_ref[k:k + 1, :] - first
        hit = (lane == lax.rem(loc, 128)) & (loc >= 0) & (loc < vocab)
        stats[me, 1 + k:2 + k, :] = jnp.sum(jnp.where(hit, picked[k].reshape(rows, 128).T, 0.0), axis=0, keepdims=True)
    st_copies = [remote(stats.at[me], st_send.at[d - 1], st_recv.at[d - 1], lax.rem(me + d, n)) for d in range(1, n)]
    for cp in st_copies:
        cp.start()
    for cp in st_copies:
        cp.wait()
    for cp in sent:
        cp.wait_send()
    total = stats[0]
    for d in range(1, n):
        total = total + stats[d]
    lse = jnp.log(total[0:1, :])
    tail_ref[0:1, :] = lse
    tail_ref[1:1 + n_cand, :] = total[1:1 + n_cand, :] * SOFT_CAP - lse


def write_kernel(t_ref, tail_ref, lse_hbm, cand_hbm, out_hbm, lse_buf, cand_buf, l_col, obuf, o_sem, t_sem):
    rows, vocab = out_hbm.shape
    lse_buf[...] = tail_ref[0:1, :]
    cand_buf[...] = tail_ref[1:1 + cand_buf.shape[0], :]
    for b in range(rows // 128):
        l_col[b * 128:(b + 1) * 128, :] = jnp.broadcast_to(tail_ref[0:1, b * 128:(b + 1) * 128], (128, 128)).T
    small = [pltpu.make_async_copy(lse_buf, lse_hbm, t_sem.at[0]), pltpu.make_async_copy(cand_buf, cand_hbm, t_sem.at[1])]
    for cp in small:
        cp.start()
    n_blk = rows // OUT_ROWS

    def out_copy(i, slot):
        return pltpu.make_async_copy(
            obuf.at[slot], out_hbm.at[pl.ds(pl.multiple_of(i * OUT_ROWS, OUT_ROWS), OUT_ROWS), :], o_sem.at[slot])

    def block(i, carry):
        slot = lax.rem(i, OUT_RING)

        @pl.when(i >= OUT_RING)
        def _():
            out_copy(i - OUT_RING, slot).wait()
        r0 = pl.multiple_of(i * OUT_ROWS, OUT_ROWS)
        col = l_col[pl.ds(r0, OUT_ROWS), :]
        tiles = 16

        def part(q, c):
            for v in range(tiles):
                t = t_ref[q * tiles + v, pl.ds(i * (OUT_ROWS // 8), OUT_ROWS // 8)].reshape(OUT_ROWS, 128)
                obuf[slot, :, pl.ds(pl.multiple_of(q * (tiles * 128) + v * 128, 128), 128)] = (t * SOFT_CAP - col).astype(jnp.bfloat16)
            return c

        lax.fori_loop(0, vocab // (128 * tiles), part, 0)
        out_copy(i, slot).start()
        return carry

    lax.fori_loop(0, n_blk, block, 0)
    for i in range(n_blk - OUT_RING, n_blk):
        out_copy(i, i % OUT_RING).wait()
    for cp in small:
        cp.wait()


def solution(mesh):
    n = mesh.shape["tp"]

    def device_step(hidden_blk, cand_ids, scale_blk, table_blk):
        rows, feat = hidden_blk.shape
        vocab, width = table_blk.shape
        n_cand = cand_ids.shape[1]
        ids_t = cand_ids.T
        dma = pltpu.SemaphoreType.DMA
        any_space = pl.BlockSpec(memory_space=pl.ANY)
        vmem = pl.BlockSpec(memory_space=pltpu.VMEM)
        capped, tail = pl.pallas_call(
            functools.partial(head_kernel, n),
            out_shape=(pltpu.VMEM((vocab // 128, rows // 8, 8, 128), jnp.float32),
                       pltpu.VMEM((8, rows), jnp.float32)),
            in_specs=[any_space] * 4,
            out_specs=(vmem, vmem),
            scratch_shapes=[
                pltpu.VMEM((RING, CHUNK, width), jnp.bfloat16),
                pltpu.VMEM((n, rows // 128, feat, 128), jnp.bfloat16),
                pltpu.VMEM((feat,), jnp.bfloat16),
                pltpu.VMEM((n, 1, feat), jnp.float32),
                pltpu.VMEM((n * feat, 128), jnp.float32),
                pltpu.VMEM((n, 8, rows), jnp.float32),
                pltpu.VMEM((n * feat, rows), jnp.bfloat16),
                pltpu.VMEM((CHUNK, rows), jnp.float32),
                pltpu.VMEM((CHUNK, rows), jnp.float32),
                pltpu.SMEM((n_cand, rows), jnp.int32),
                pltpu.VMEM((n_cand, rows), jnp.int32),
                pltpu.VMEM((n_cand, rows), jnp.int32),
                pltpu.VMEM((n_cand, rows // 8, 8, 128), jnp.float32),
                pltpu.VMEM((n, 8, rows), jnp.float32),
                dma((RING,)), dma((rows // 128 + 3,)), dma((n - 1,)), dma((n - 1,)),
                dma((3, rows // 128)), dma((3, rows // 128)), dma((4, rows // 128)), dma((4, rows // 128)),
                dma((n - 1,)), dma((n - 1,)),
            ],
            compiler_params=pltpu.CompilerParams(
                collective_id=0, has_side_effects=True, vmem_limit_bytes=31 * 2**20),
        )(hidden_blk.T, scale_blk, ids_t, table_blk)
        lse, cand, logp = pl.pallas_call(
            write_kernel,
            out_shape=(jax.ShapeDtypeStruct((1, rows), jnp.float32),
                       jax.ShapeDtypeStruct((n_cand, rows), jnp.float32),
                       jax.ShapeDtypeStruct((rows, vocab), jnp.bfloat16)),
            in_specs=[vmem, vmem],
            out_specs=(any_space,) * 3,
            scratch_shapes=[pltpu.VMEM((1, rows), jnp.float32),
                            pltpu.VMEM((n_cand, rows), jnp.float32),
                            pltpu.VMEM((rows, 128), jnp.float32),
                            pltpu.VMEM((OUT_RING, OUT_ROWS, vocab), jnp.bfloat16),
                            dma((OUT_RING,)), dma((2,))],
            compiler_params=pltpu.CompilerParams(vmem_limit_bytes=31 * 2**20),
        )(pltpu.with_memory_space_constraint(capped, pltpu.VMEM),
          pltpu.with_memory_space_constraint(tail, pltpu.VMEM))
        return lse.reshape(rows), cand.T, logp

    return jax.shard_map(
        device_step,
        mesh=mesh,
        in_specs=(P("dp", "tp"), P("dp", None), P("tp"), P("tp", None)),
        out_specs=(P("dp"), P("dp", None), P("dp", "tp")),
        check_vma=False,
    )
```
